128 devices in a mesh: groups: 4 (over y, x), lat: 32 (over z, core).
Axes of the slice: x: 2, y: 2, z: 16, core: 2. Of those that a mesh axis runs over, the one named last changes fastest.
The devices are a block of a 8x8x16 slice.
Arguments:
- inputs: bfloat16 [2048, 4608], P('groups', 'lat'), parts along dimension 0, may hold values from -6 to 6
- w_enc: bfloat16 [18432, 16384], P('groups', 'lat'), parts along dimension 0, may hold values from -0.09375 to 0.09375
- b_enc: float32 [65536], P(('groups', 'lat')), parts along dimension 0, may hold values from -3 to 3
- thresholds: float32 [65536], P(('groups', 'lat')), parts along dimension 0, may hold values from 0.1 to 4
- w_dec: bfloat16 [65536, 4608], P(('groups', 'lat')), parts along dimension 0, may hold values from -0.1875 to 0.1875
- b_dec: bfloat16 [18432], P(('groups', 'lat')), parts along dimension 0, may hold values from -5 to 5
- sparsity: float32 [4], P('groups'), parts along dimension 0, may hold values from 1 to 4
Outputs:
- grad_enc: bfloat16 [18432, 16384], P('groups', 'lat'), parts along dimension 0
- grad_b_enc: float32 [65536], P(('groups', 'lat')), parts along dimension 0
- grad_dec: bfloat16 [65536, 4608], P(('groups', 'lat')), parts along dimension 0
- grad_b_dec: float32 [18432], P(('groups', 'lat')), parts along dimension 0
- loss_terms: float32 [8], P('groups'), parts along dimension 0
The draws below stay inside these ranges and needn't reach their ends.
There are 4 independent parts, one for each index of `groups`. The reference program is written for one: setup_inputs(seed, part) draws one part's arguments, and reference() takes and returns one part's arrays. A program takes and returns all parts, laid end to end along the dimension named above; each array names one. Nothing has to cross between parts.
All inputs are finite; a program needn't handle non-finite values.
Results may differ from the reference program's by a relative error of at most 0.006.
Values may be sent and summed in bfloat16 or wider, within the bound.
No kernel may reach another device: no remote copies, remote signals or barrier semaphores. Data moves between devices by JAX's collectives and lax.ppermute only.
A program may use at most 128 MiB of HBM per device.

```python
import math
import jax
import jax.numpy as jnp
from jax import lax

D = 4608
LAT_DEV = 512
ROWS = 512
LATENTS = 16384


def draw_thresholds(key, part):
    blocks = LATENTS // LAT_DEV
    key_level = jax.random.fold_in(key, 11)
    key_inner = jax.random.fold_in(key, 23)
    key_pick = jax.random.fold_in(key, 37)
    levels = jnp.exp(jax.random.uniform(key_level, (blocks, 1), jnp.float32, math.log(0.25), math.log(2.5)))
    chosen = jax.random.randint(key_pick, (), 0, blocks)
    levels = jnp.where(jnp.arange(blocks).reshape(blocks, 1) == chosen, jnp.float32(0.25), levels)
    inner = jnp.exp(jax.random.uniform(key_inner, (blocks, LAT_DEV), jnp.float32, math.log(0.4), math.log(1.6)))
    return (levels * inner).reshape(LATENTS).astype(jnp.float32)


def with_spikes(values, own_key, source, target, shards_of, factor):
    owner, partner = [(jnp.arange(values.shape[dim]) // (values.shape[dim] // shards_of)).reshape([-1 if axis == dim else 1 for axis in range(values.ndim)]) for dim in (source, target)]
    chosen = jax.random.permutation(own_key, shards_of)[partner]
    strong = (owner == chosen) | (owner == (partner + shards_of // 2) % shards_of)
    return jnp.where(strong, factor * values, values)


def level_of(stream_key, shape, shards, least, high):
    level = 1.0
    for position, shards_of in shards:
        draws = jax.random.uniform(jax.random.fold_in(jax.random.fold_in(stream_key, 6), position), (shards_of,), jnp.float32, least / len(shards), high / len(shards))
        level = level * jnp.repeat(jnp.exp(draws), shape[position] // shards_of).reshape((-1,) + (1,) * (len(shape) - 1 - position))
    return level


def normal_values(stream_key, extent, deviation, bound, shards=(), held_as=jnp.bfloat16):
    array = deviation * jax.random.normal(stream_key, extent, jnp.float32)
    if shards:
        array = array * level_of(stream_key, extent, shards, -0.22, 0.18)
    return jnp.clip(array, -bound, bound).astype(held_as)


def gaussian_with(rng, shape, deviation, reach, cuts, heavy, kind=jnp.bfloat16):
    entries = deviation * jax.random.normal(rng, shape, jnp.float32)
    if cuts:
        entries = entries * level_of(rng, shape, cuts, -0.22, 0.18)
    return jnp.clip(with_spikes(entries, jax.random.fold_in(rng, 3), *heavy), -reach, reach).astype(kind)


def setup_inputs(seed: int = 0, part: int = 0) -> dict:
    splits = jax.random.split(jax.random.key(seed), 8)
    own_keys = jax.random.split(jax.random.fold_in(splits[7], part), 8)
    return {
        "inputs": normal_values(own_keys[0], (ROWS, D), 1.0, 6.0, ((1, 32),)),
        "w_enc": normal_values(own_keys[1], (D, LATENTS), D ** -0.5, 0.09375, ((1, 32),)),
        "b_enc": normal_values(own_keys[2], (LATENTS,), 0.5, 3.0, ((0, 32),), jnp.float32),
        "thresholds": draw_thresholds(jax.random.fold_in(jax.random.fold_in(splits[7], part), 71), part),
        "w_dec": gaussian_with(own_keys[4], (LATENTS, D), (LATENTS // 4) ** -0.5, 0.1875, ((0, 32),), (0, 1, 32, 2.75)),
        "b_dec": normal_values(own_keys[5], (D,), 1.0, 5.0, ((0, 32),)),
        "sparsity": jnp.clip(jax.random.uniform(own_keys[6], (1,), jnp.float32, 1.0, 4.0), 1.0, 4.0),
    }


def reference(inputs, w_enc, b_enc, thresholds, w_dec, b_dec, sparsity):
    rows = inputs.shape[0]
    pre = jnp.dot(inputs, w_enc, preferred_element_type=jnp.float32) + b_enc
    gate = jax.nn.sigmoid((pre - thresholds) / 0.05)
    feats = (pre * gate).astype(jnp.bfloat16)
    recon = jnp.dot(feats, w_dec, preferred_element_type=jnp.float32) + b_dec.astype(jnp.float32)
    err = recon - inputs.astype(jnp.float32)
    scaled = (2.0 / rows) * err
    error_bf = scaled.astype(jnp.bfloat16)
    grad_b_dec = jnp.sum(scaled, axis=0)
    grad_dec = lax.dot_general(feats, error_bf, (((0,), (0,)), ((), ())), preferred_element_type=jnp.float32).astype(jnp.bfloat16)
    g_feats = lax.dot_general(error_bf, w_dec, (((1,), (1,)), ((), ())), preferred_element_type=jnp.float32)
    g_pre = g_feats * (gate + pre * gate * (1.0 - gate) / 0.05)
    g_pre_bf = g_pre.astype(jnp.bfloat16)
    grad_b_enc = jnp.sum(g_pre, axis=0)
    grad_enc = lax.dot_general(inputs, g_pre_bf, (((0,), (0,)), ((), ())), preferred_element_type=jnp.float32).astype(jnp.bfloat16)
    loss_terms = jnp.stack([jnp.sum(err * err) / (rows * D), sparsity[0] * jnp.sum(gate) / (rows * LATENTS)])
    return grad_enc, grad_b_enc, grad_dec, grad_b_dec, loss_terms
```

```python
import jax
import jax.numpy as jnp
from jax import lax
from jax.experimental import pallas as pl
from jax.experimental.pallas import tpu as pltpu
from jax.sharding import Mesh
from jax.sharding import PartitionSpec as P

LAT = ("lat_0", "lat_1")
GROUPS_LAT = ("groups", "lat_0", "lat_1")
F32 = jnp.float32
BF = jnp.bfloat16


def ring(a, step):
    n = lax.axis_size("lat_0")
    return lax.ppermute(a, "lat_0", [(z, (z + step) % n) for z in range(n)])


def swap(a):
    return lax.ppermute(a, "lat_1", [(0, 1), (1, 0)])


def after(a, b):
    return lax.optimization_barrier((a, b))[0]


def gather_chips(block, height, z, n):
    half = n // 2
    rest = block.shape[0] - height
    full = jnp.zeros((n, height, block.shape[1]), block.dtype)
    tail = jnp.zeros((n, rest, block.shape[1]), block.dtype) if rest else None

    def store(full, tail, piece, chip):
        at = (chip % n, 0, 0)
        full = lax.dynamic_update_slice(full, piece[None, :height], at)
        if rest:
            tail = lax.dynamic_update_slice(tail, piece[None, height:], at)
        return full, tail

    full, tail = store(full, tail, block, z)
    up = down = last = block
    for k in range(1, half + 1):
        up = ring(after(up, last), 1)
        full, tail = store(full, tail, up, z - k)
        last = up
        if k < half:
            down = ring(down, -1)
            full, tail = store(full, tail, down, z + k)
            last = down
    return full, tail


def scatter_sum(mine, theirs, z, n):
    half = n // 2

    def take(chip):
        at = (chip % n, 0, 0)
        size = (1, *mine.shape[1:])
        return (
            lax.dynamic_slice(mine, at, size)[0]
            + lax.dynamic_slice(theirs, at, size)[0].astype(F32)
        )

    up = ring(take(z + half).astype(BF), 1)
    down = ring(take(z - half + 1).astype(BF), -1)
    for j in range(half - 1, 0, -1):
        up, down = lax.optimization_barrier((up, down))
        up = ring((take(z + j) + up.astype(F32)).astype(BF), 1)
        if j > 1:
            down = ring((take(z - j + 1) + down.astype(F32)).astype(BF), -1)
    return take(z) + up.astype(F32) + down.astype(F32)


def as_parts(v):
    parts = []
    for _ in range(3):
        part = lax.reduce_precision(v, 8, 7)
        parts.append(part.astype(BF))
        v = v - part
    return parts


def joined(c, a, b):
    k, cols, rows = a.shape
    first = jnp.where(c == 0, a, b).reshape(k, 1, cols, rows)
    second = jnp.where(c == 0, b, a).reshape(k, 1, cols, rows)
    return jnp.concatenate([first, second], 1).reshape(2 * k * cols, rows)


def step_chips(n, cols):
    k = 1
    while 2 * k * cols % 128:
        k += 1
    return k


SMEM_SPEC = pl.BlockSpec(memory_space=pltpu.SMEM)


def whole(shape):
    return pl.BlockSpec(shape, lambda i: (0,) * len(shape))


def decode(core, w_dec, feats, n):
    latents, width = w_dec.shape
    rows = feats.shape[1]
    cols = width // (2 * n)
    k = step_chips(n, cols)

    def kernel(core_ref, w_ref, f_ref, mine_ref, theirs_ref):
        c = core_ref[0]
        p = lax.dot_general(
            w_ref[...], f_ref[...], (((0,), (0,)), ((), ())), preferred_element_type=F32
        ).reshape(k, 2, cols, rows)
        mine_ref[...] = jnp.where(c == 0, p[:, 0], p[:, 1])
        theirs_ref[...] = jnp.where(c == 0, p[:, 1], p[:, 0]).astype(BF)

    block = pl.BlockSpec((k, cols, rows), lambda i: (i, 0, 0))
    return pl.pallas_call(
        kernel,
        grid=(n // k,),
        in_specs=[
            SMEM_SPEC,
            pl.BlockSpec((latents, 2 * k * cols), lambda i: (0, i)),
            whole((latents, rows)),
        ],
        out_specs=[block, block],
        out_shape=[
            jax.ShapeDtypeStruct((n, cols, rows), F32),
            jax.ShapeDtypeStruct((n, cols, rows), BF),
        ],
        name="decode",
    )(core, w_dec, feats)


def backward(core, e_a, e_b, w_dec, feats, pre, gate):
    n, cols, rows = e_a.shape
    latents, width = w_dec.shape
    k = step_chips(n, cols)

    def kernel(core_ref, a_ref, b_ref, w_ref, f_ref, pre_ref, gate_ref, dec_ref, g_ref, bias_ref, acc):
        i = pl.program_id(0)
        e = joined(core_ref[0], a_ref[...], b_ref[...])
        dec_ref[...] = lax.dot_general(
            f_ref[...], e, (((1,), (1,)), ((), ())), preferred_element_type=F32
        ).astype(BF)
        part = jnp.dot(w_ref[...], e, preferred_element_type=F32)

        @pl.when(i == 0)
        def _():
            acc[...] = part

        @pl.when(i > 0)
        def _():
            acc[...] += part

        @pl.when(i == n // k - 1)
        def _():
            gate = gate_ref[...]
            g = acc[...] * (gate + pre_ref[...] * gate * (1.0 - gate) / 0.05)
            g_ref[...] = g.astype(BF)
            bias_ref[...] = jnp.sum(g, axis=1, keepdims=True)

    block = pl.BlockSpec((k, cols, rows), lambda i: (i, 0, 0))
    tall = pl.BlockSpec((latents, 2 * k * cols), lambda i: (0, i))
    square = whole((latents, rows))
    return pl.pallas_call(
        kernel,
        grid=(n // k,),
        in_specs=[SMEM_SPEC, block, block, tall, square, square, square],
        out_specs=[tall, square, whole((latents, 1))],
        out_shape=[
            jax.ShapeDtypeStruct((latents, width), BF),
            jax.ShapeDtypeStruct((latents, rows), BF),
            jax.ShapeDtypeStruct((latents, 1), F32),
        ],
        scratch_shapes=[pltpu.VMEM((latents, rows), F32)],
        name="backward",
    )(core, e_a, e_b, w_dec, feats, pre, gate)


def encoder_grad(core, x_a, x_b, g_pre):
    n, cols, rows = x_a.shape
    latents = g_pre.shape[0]
    k = step_chips(n, cols)

    def kernel(core_ref, a_ref, b_ref, g_ref, out_ref):
        x = joined(core_ref[0], a_ref[...], b_ref[...])
        out_ref[...] = lax.dot_general(
            x, g_ref[...], (((1,), (1,)), ((), ())), preferred_element_type=F32
        ).astype(BF)

    block = pl.BlockSpec((k, cols, rows), lambda i: (i, 0, 0))
    return pl.pallas_call(
        kernel,
        grid=(n // k,),
        in_specs=[SMEM_SPEC, block, block, whole((latents, rows))],
        out_specs=pl.BlockSpec((2 * k * cols, latents), lambda i: (i, 0)),
        out_shape=jax.ShapeDtypeStruct((2 * n * cols, latents), BF),
        name="encoder_grad",
    )(core, x_a, x_b, g_pre)


def on_device(inputs, w_enc, b_enc, thresholds, w_dec, b_dec, sparsity):
    n = lax.axis_size("lat_0")
    z = lax.axis_index("lat_0")
    c = lax.axis_index("lat_1")
    core = c.astype(jnp.int32).reshape(1)
    rows, cols = inputs.shape
    width = w_enc.shape[0]
    latents = w_enc.shape[1]
    x_own = inputs.T

    def half_of(w, k):
        w = w.reshape(n, 2, cols, latents)
        return lax.dynamic_index_in_dim(w, k, 1, False).reshape(n * cols, latents)

    def over_columns(w, a):
        a = a.reshape(n * cols, rows)
        return lax.dot_general(w, a, (((0,), (0,)), ((), ())), preferred_element_type=F32)

    x_a, _ = gather_chips(x_own, cols, z, n)
    x_b = swap(x_a)
    pre = (
        over_columns(half_of(w_enc, c), x_a)
        + over_columns(half_of(w_enc, 1 - c), x_b)
        + b_enc[:, None]
    )
    gate = jax.nn.sigmoid((pre - thresholds[:, None]) / 0.05)
    feats = (pre * gate).astype(BF)
    count = jnp.sum(gate)

    mine, theirs = decode(core, w_dec, feats, n)
    recon = scatter_sum(mine, swap(theirs), z, n)
    err = recon + b_dec.astype(F32)[:, None] - x_own.astype(F32)
    scaled = 2.0 / rows * err
    grad_b_dec = jnp.sum(scaled, axis=1)

    parts = jnp.stack(as_parts(jnp.sum(err * err)) + as_parts(count))
    beside = jnp.broadcast_to(jnp.pad(parts, (0, 16 - parts.size))[:, None], (16, rows))
    block = jnp.concatenate([scaled.astype(BF), beside], 0)
    e_a, sums = gather_chips(block, cols, z, n)
    e_b = swap(e_a)
    sums = jnp.sum(sums[:, :6, :128].astype(F32).reshape(n, 2, 3, 128), axis=(0, 2))
    sums = (sums + swap(sums))[:, 0]

    grad_dec, g_pre, grad_b_enc = backward(core, e_a, e_b, w_dec, feats, pre, gate)
    grad_enc = encoder_grad(core, x_a, x_b, g_pre)
    loss_terms = jnp.stack(
        [sums[0] / (rows * width), sparsity[0] * sums[1] / (rows * latents * 2 * n)]
    )
    return (grad_enc, grad_b_enc[:, 0], grad_dec, grad_b_dec, loss_terms)


def solution(mesh):
    lat = mesh.shape["lat"]
    finer = Mesh(
        mesh.devices.reshape(mesh.shape["groups"], lat // 2, 2), ("groups", "lat_0", "lat_1")
    )
    in_specs = (
        P("groups", LAT),
        P("groups", LAT),
        P(GROUPS_LAT),
        P(GROUPS_LAT),
        P(GROUPS_LAT, None),
        P(GROUPS_LAT),
        P("groups"),
    )
    out_specs = (P("groups", LAT), P(GROUPS_LAT), P(GROUPS_LAT, None), P(GROUPS_LAT), P("groups"))
    return jax.shard_map(
        on_device, mesh=finer, in_specs=in_specs, out_specs=out_specs, check_vma=False
    )
```

```python
import jax
import jax.numpy as jnp
from jax import lax
from jax.experimental import pallas as pl
from jax.experimental.pallas import tpu as pltpu
from jax.sharding import Mesh
from jax.sharding import PartitionSpec as P

LAT = ("lat_0", "lat_1")
GROUPS_LAT = ("groups", "lat_0", "lat_1")
F32 = jnp.float32
BF = jnp.bfloat16


def ring(a, step):
    n = lax.axis_size("lat_0")
    return lax.ppermute(a, "lat_0", [(z, (z + step) % n) for z in range(n)])


def swap(a):
    return lax.ppermute(a, "lat_1", [(0, 1), (1, 0)])


def after(a, b):
    return lax.optimization_barrier((a, b))[0]


def gather_chips(block, height, z, n, work=None):
    done = None
    half = n // 2
    rest = block.shape[0] - height
    full = jnp.zeros((n, height, block.shape[1]), block.dtype)
    tail = jnp.zeros((n, rest, block.shape[1]), block.dtype) if rest else None

    def store(full, tail, piece, chip):
        at = (chip % n, 0, 0)
        full = lax.dynamic_update_slice(full, piece[None, :height], at)
        if rest:
            tail = lax.dynamic_update_slice(tail, piece[None, height:], at)
        return full, tail

    full, tail = store(full, tail, block, z)
    up = down = last = block
    for k in range(1, half + 1):
        up = after(up, last)
        if work is not None and k == 5:
            up = after(up, done)
        up = ring(up, 1)
        full, tail = store(full, tail, up, z - k)
        last = up
        if work is not None and k == 3:
            done = work(last)
        if k < half:
            down = ring(down, -1)
            full, tail = store(full, tail, down, z + k)
            last = down
    return full, tail, done


def scatter_sum(mine, theirs, z, n):
    half = n // 2

    def take(chip):
        at = (chip % n, 0, 0)
        size = (1, *mine.shape[1:])
        return (
            lax.dynamic_slice(mine, at, size)[0]
            + lax.dynamic_slice(theirs, at, size)[0].astype(F32)
        )

    up = ring(take(z + half).astype(BF), 1)
    down = ring(take(z - half + 1).astype(BF), -1)
    for j in range(half - 1, 0, -1):
        up, down = lax.optimization_barrier((up, down))
        up = ring((take(z + j) + up.astype(F32)).astype(BF), 1)
        if j > 1:
            down = ring((take(z - j + 1) + down.astype(F32)).astype(BF), -1)
    return take(z), up, down


def joined(c, a_ref, b_ref, both_ref):
    k, cols, rows = a_ref.shape
    both_ref[:, pl.ds(c, 1)] = a_ref[...].reshape(k, 1, cols, rows)
    both_ref[:, pl.ds(1 - c, 1)] = b_ref[...].reshape(k, 1, cols, rows)
    return both_ref[...].reshape(2 * k * cols, rows)


def step_chips(n, cols):
    k = 1
    while 2 * k * cols % 128:
        k += 1
    return k


EXTRA = 16
SMEM_SPEC = pl.BlockSpec(memory_space=pltpu.SMEM)


def whole(shape):
    return pl.BlockSpec(shape, lambda i: (0,) * len(shape))


def decode(core, w_dec, feats, n):
    latents, width = w_dec.shape
    rows = feats.shape[1]
    cols = width // (2 * n)
    k = step_chips(n, cols)

    def kernel(core_ref, w_ref, f_ref, mine_ref, theirs_ref, both_ref):
        c = core_ref[0]
        both_ref[...] = lax.dot_general(
            w_ref[...], f_ref[...], (((0,), (0,)), ((), ())), preferred_element_type=F32
        ).reshape(k, 2, cols, rows)
        mine_ref[...] = both_ref[:, pl.ds(c, 1)].reshape(k, cols, rows)
        theirs_ref[...] = both_ref[:, pl.ds(1 - c, 1)].reshape(k, cols, rows).astype(BF)

    block = pl.BlockSpec((k, cols, rows), lambda i: (i, 0, 0))
    return pl.pallas_call(
        kernel,
        grid=(n // k,),
        in_specs=[
            SMEM_SPEC,
            pl.BlockSpec((latents, 2 * k * cols), lambda i: (0, i)),
            whole((latents, rows)),
        ],
        out_specs=[block, block],
        out_shape=[
            jax.ShapeDtypeStruct((n, cols, rows), F32),
            jax.ShapeDtypeStruct((n, cols, rows), BF),
        ],
        scratch_shapes=[pltpu.VMEM((k, 2, cols, rows), F32)],
        name="decode",
    )(core, w_dec, feats)


def error_block(own, up, down, x, bias, count):
    cols, rows = x.shape

    def kernel(own_ref, up_ref, down_ref, x_ref, bias_ref, count_ref, out_ref, grad_ref):
        recon = own_ref[...] + up_ref[...].astype(F32) + down_ref[...].astype(F32)
        err = recon + bias_ref[...] - x_ref[...].astype(F32)
        scaled = 2.0 / rows * err
        out_ref[:cols, :] = scaled.astype(BF)
        grad_ref[...] = jnp.sum(scaled, axis=1, keepdims=True)
        parts = []
        for v in (jnp.sum(err * err, axis=0, keepdims=True), count_ref[...]):
            for _ in range(3):
                part = v.astype(BF)
                parts.append(part.astype(F32))
                v = v - parts[-1]
        row = lax.broadcasted_iota(jnp.int32, (EXTRA, rows), 0)
        extra = jnp.zeros((EXTRA, rows), F32)
        for k, part in enumerate(parts):
            extra = jnp.where(row == k, part, extra)
        out_ref[cols:, :] = extra.astype(BF)

    return pl.pallas_call(
        kernel,
        out_shape=[
            jax.ShapeDtypeStruct((cols + EXTRA, rows), BF),
            jax.ShapeDtypeStruct((cols, 1), F32),
        ],
        name="error_block",
    )(own, up, down, x, bias, count)


def backward(core, e_a, e_b, w_dec, feats, pre, gate):
    n, cols, rows = e_a.shape
    latents, width = w_dec.shape
    k = step_chips(n, cols)

    def kernel(core_ref, a_ref, b_ref, w_ref, f_ref, pre_ref, gate_ref, dec_ref, g_ref, bias_ref, acc, both_ref):
        i = pl.program_id(0)
        e = joined(core_ref[0], a_ref, b_ref, both_ref)
        dec_ref[...] = lax.dot_general(
            f_ref[...], e, (((1,), (1,)), ((), ())), preferred_element_type=F32
        ).astype(BF)
        part = jnp.dot(w_ref[...], e, preferred_element_type=F32)

        @pl.when(i == 0)
        def _():
            acc[...] = part

        @pl.when(i > 0)
        def _():
            acc[...] += part

        @pl.when(i == n // k - 1)
        def _():
            gate = gate_ref[...]
            g = acc[...] * (gate + pre_ref[...] * gate * (1.0 - gate) / 0.05)
            g_ref[...] = g.astype(BF)
            lanes = sum(g[:, b : b + 128] for b in range(0, rows, 128))
            bias_ref[...] = jnp.sum(lanes.T, axis=0, keepdims=True)

    block = pl.BlockSpec((k, cols, rows), lambda i: (i, 0, 0))
    tall = pl.BlockSpec((latents, 2 * k * cols), lambda i: (0, i))
    square = whole((latents, rows))
    return pl.pallas_call(
        kernel,
        grid=(n // k,),
        in_specs=[SMEM_SPEC, block, block, tall, square, square, square],
        out_specs=[tall, square, whole((1, latents))],
        out_shape=[
            jax.ShapeDtypeStruct((latents, width), BF),
            jax.ShapeDtypeStruct((latents, rows), BF),
            jax.ShapeDtypeStruct((1, latents), F32),
        ],
        scratch_shapes=[
            pltpu.VMEM((latents, rows), F32),
            pltpu.VMEM((k, 2, cols, rows), BF),
        ],
        name="backward",
    )(core, e_a, e_b, w_dec, feats, pre, gate)


def encoder_grad(core, x_a, x_b, g_pre):
    n, cols, rows = x_a.shape
    latents = g_pre.shape[0]
    k = step_chips(n, cols)

    def kernel(core_ref, a_ref, b_ref, g_ref, out_ref, both_ref):
        x = joined(core_ref[0], a_ref, b_ref, both_ref)
        out_ref[...] = lax.dot_general(
            x, g_ref[...], (((1,), (1,)), ((), ())), preferred_element_type=F32
        ).astype(BF)

    block = pl.BlockSpec((k, cols, rows), lambda i: (i, 0, 0))
    return pl.pallas_call(
        kernel,
        grid=(n // k,),
        in_specs=[SMEM_SPEC, block, block, whole((latents, rows))],
        out_specs=pl.BlockSpec((2 * k * cols, latents), lambda i: (i, 0)),
        out_shape=jax.ShapeDtypeStruct((2 * n * cols, latents), BF),
        scratch_shapes=[pltpu.VMEM((k, 2, cols, rows), BF)],
        name="encoder_grad",
    )(core, x_a, x_b, g_pre)


def on_device(inputs, w_enc, b_enc, thresholds, w_dec, b_dec, sparsity):
    n = lax.axis_size("lat_0")
    z = lax.axis_index("lat_0")
    c = lax.axis_index("lat_1")
    core = c.astype(jnp.int32).reshape(1)
    rows, cols = inputs.shape
    width = w_enc.shape[0]
    latents = w_enc.shape[1]
    x_own = inputs.T

    def half_of(w, k):
        w = w.reshape(n, 2, cols, latents)
        return lax.dynamic_index_in_dim(w, k, 1, False).reshape(n * cols, latents)

    def over_columns(w, a):
        a = a.reshape(n * cols, rows)
        return lax.dot_general(w, a, (((0,), (0,)), ((), ())), preferred_element_type=F32)

    def encoder_halves(token):
        w = after(w_enc, token)
        return half_of(w, c), half_of(w, 1 - c)

    x_a, _, (w_a, w_b) = gather_chips(x_own, cols, z, n, encoder_halves)
    x_b = swap(x_a)
    pre = over_columns(w_a, x_a) + over_columns(w_b, x_b) + b_enc[:, None]
    gate = jax.nn.sigmoid((pre - thresholds[:, None]) / 0.05)
    feats = (pre * gate).astype(BF)
    count = jnp.sum(gate, axis=0, keepdims=True)

    mine, theirs = decode(core, w_dec, feats, n)
    own, up, down = scatter_sum(mine, swap(theirs), z, n)
    block, grad_b_dec = error_block(own, up, down, x_own, b_dec.astype(F32)[:, None], count)
    e_a, sums, _ = gather_chips(block, cols, z, n)
    e_b = swap(e_a)
    sums = jnp.sum(sums[:, :6].astype(F32).reshape(n, 2, 3, rows), axis=(0, 2, 3))
    sums = jnp.broadcast_to(sums[:, None], (2, 128))
    sums = (sums + swap(sums))[:, 0]

    grad_dec, g_pre, grad_b_enc = backward(core, e_a, e_b, w_dec, feats, pre, gate)
    grad_enc = encoder_grad(core, x_a, x_b, g_pre)
    loss_terms = jnp.stack(
        [sums[0] / (rows * width), sparsity[0] * sums[1] / (rows * latents * 2 * n)]
    )
    return (grad_enc, grad_b_enc[0], grad_dec, grad_b_dec[:, 0], loss_terms)


def solution(mesh):
    lat = mesh.shape["lat"]
    finer = Mesh(
        mesh.devices.reshape(mesh.shape["groups"], lat // 2, 2), ("groups", "lat_0", "lat_1")
    )
    in_specs = (
        P("groups", LAT),
        P("groups", LAT),
        P(GROUPS_LAT),
        P(GROUPS_LAT),
        P(GROUPS_LAT, None),
        P(GROUPS_LAT),
        P("groups"),
    )
    out_specs = (P("groups", LAT), P(GROUPS_LAT), P(GROUPS_LAT, None), P(GROUPS_LAT), P("groups"))
    return jax.shard_map(
        on_device, mesh=finer, in_specs=in_specs, out_specs=out_specs, check_vma=False
    )
```

```python
import jax
import jax.numpy as jnp
from jax import lax
from jax.experimental import pallas as pl
from jax.experimental.pallas import tpu as pltpu
from jax.sharding import Mesh
from jax.sharding import PartitionSpec as P

LAT = ("lat_0", "lat_1")
GROUPS_LAT = ("groups", "lat_0", "lat_1")
F32 = jnp.float32
BF = jnp.bfloat16


def ring(a, step):
    n = lax.axis_size("lat_0")
    return lax.ppermute(a, "lat_0", [(z, (z + step) % n) for z in range(n)])


def swap(a):
    return lax.ppermute(a, "lat_1", [(0, 1), (1, 0)])


def after(a, b):
    return lax.optimization_barrier((a, b))[0]


def gather_chips(block, z, n, work=None):
    half = n // 2
    full = jnp.zeros((n, *block.shape), block.dtype)
    done = None

    def store(full, piece, chip):
        return lax.dynamic_update_slice(full, piece[None], (chip % n, 0, 0))

    full = store(full, block, z)
    up = down = last = block
    for k in range(1, half + 1):
        up = after(up, last)
        if work is not None and k == 5:
            up = after(up, done)
        up = ring(up, 1)
        full = store(full, up, z - k)
        last = up
        if work is not None and k == 3:
            done = work(last)
        if k < half:
            down = ring(down, -1)
            full = store(full, down, z + k)
            last = down
    return full, done


def scatter_sum(mine, theirs, z, n):
    half = n // 2

    def take(chip):
        at = (chip % n, 0, 0)
        size = (1, *mine.shape[1:])
        return (
            lax.dynamic_slice(mine, at, size)[0]
            + lax.dynamic_slice(theirs, at, size)[0].astype(F32)
        )

    up = ring(take(z + half).astype(BF), 1)
    down = ring(take(z - half + 1).astype(BF), -1)
    for j in range(half - 1, 0, -1):
        up, down = lax.optimization_barrier((up, down))
        up = ring((take(z + j) + up.astype(F32)).astype(BF), 1)
        if j > 1:
            down = ring((take(z - j + 1) + down.astype(F32)).astype(BF), -1)
    return take(z), up, down


def joined(c, a_ref, b_ref, both_ref):
    k, _, cols, rows = both_ref.shape
    both_ref[:, pl.ds(c, 1)] = a_ref[:, :cols, :].reshape(k, 1, cols, rows)
    both_ref[:, pl.ds(1 - c, 1)] = b_ref[:, :cols, :].reshape(k, 1, cols, rows)
    return both_ref[...].reshape(2 * k * cols, rows)


def step_chips(n, cols):
    k = 1
    while 2 * k * cols % 128:
        k += 1
    return k


EXTRA = 8
SMEM_SPEC = pl.BlockSpec(memory_space=pltpu.SMEM)


def whole(shape):
    return pl.BlockSpec(shape, lambda i: (0,) * len(shape))


def decode(core, w_dec, feats, n):
    latents, width = w_dec.shape
    rows = feats.shape[1]
    cols = width // (2 * n)
    k = step_chips(n, cols)

    def kernel(core_ref, w_ref, f_ref, mine_ref, theirs_ref, both_ref):
        c = core_ref[0]
        both_ref[...] = lax.dot_general(
            w_ref[...], f_ref[...], (((0,), (0,)), ((), ())), preferred_element_type=F32
        ).reshape(k, 2, cols, rows)
        mine_ref[...] = both_ref[:, pl.ds(c, 1)].reshape(k, cols, rows)
        theirs_ref[...] = both_ref[:, pl.ds(1 - c, 1)].reshape(k, cols, rows).astype(BF)

    block = pl.BlockSpec((k, cols, rows), lambda i: (i, 0, 0))
    return pl.pallas_call(
        kernel,
        grid=(n // k,),
        in_specs=[
            SMEM_SPEC,
            pl.BlockSpec((latents, 2 * k * cols), lambda i: (0, i)),
            whole((latents, rows)),
        ],
        out_specs=[block, block],
        out_shape=[
            jax.ShapeDtypeStruct((n, cols, rows), F32),
            jax.ShapeDtypeStruct((n, cols, rows), BF),
        ],
        scratch_shapes=[pltpu.VMEM((k, 2, cols, rows), F32)],
        name="decode",
    )(core, w_dec, feats)


def error_block(own, up, down, x, bias, count):
    cols, rows = x.shape

    def kernel(own_ref, up_ref, down_ref, x_ref, bias_ref, count_ref, out_ref, grad_ref):
        recon = own_ref[...] + up_ref[...].astype(F32) + down_ref[...].astype(F32)
        err = recon + bias_ref[...] - x_ref[...].astype(F32)
        scaled = 2.0 / rows * err
        out_ref[:cols, :] = scaled.astype(BF)
        grad_ref[...] = jnp.sum(scaled, axis=1, keepdims=True)
        parts = []
        for v in (jnp.sum(err * err, axis=0, keepdims=True), count_ref[...]):
            for _ in range(3):
                part = v.astype(BF)
                parts.append(part.astype(F32))
                v = v - parts[-1]
        row = lax.broadcasted_iota(jnp.int32, (EXTRA, rows), 0)
        extra = jnp.zeros((EXTRA, rows), F32)
        for k, part in enumerate(parts):
            extra = jnp.where(row == k, part, extra)
        out_ref[cols:, :] = extra.astype(BF)

    return pl.pallas_call(
        kernel,
        out_shape=[
            jax.ShapeDtypeStruct((cols + EXTRA, rows), BF),
            jax.ShapeDtypeStruct((cols, 1), F32),
        ],
        compiler_params=pltpu.CompilerParams(vmem_limit_bytes=12 << 20),
        name="error_block",
    )(own, up, down, x, bias, count)


def backward(core, sparsity, e_a, e_b, x_a, x_b, w_dec, feats, slope):
    n, cols, rows = x_a.shape
    latents, width = w_dec.shape
    k = step_chips(n, cols)
    steps = n // k
    wide = 2 * k * cols

    def kernel(
        core_ref, sparsity_ref, ea_ref, eb_ref, xa_ref, xb_ref, w_ref, f_ref, slope_ref,
        dec_ref, enc_ref, bias_ref, loss_ref, acc, g_ref, both_ref, sums_ref,
    ):
        i = pl.program_id(0)

        @pl.when(i == 0)
        def _():
            acc[...] = jnp.zeros_like(acc)
            sums_ref[...] = jnp.zeros_like(sums_ref)

        @pl.when(i < steps)
        def _():
            e = joined(core_ref[0], ea_ref, eb_ref, both_ref)
            dec_ref[...] = lax.dot_general(
                f_ref[...], e, (((1,), (1,)), ((), ())), preferred_element_type=F32
            ).astype(BF)
            acc[...] += jnp.dot(w_ref[...], e, preferred_element_type=F32)
            for q in range(k):
                sums_ref[...] += ea_ref[q, cols:, :].astype(F32) + eb_ref[q, cols:, :].astype(F32)

        @pl.when(i == steps - 1)
        def _():
            g = acc[...] * slope_ref[...]
            g_ref[...] = g.astype(BF)
            lanes = sum(g[:, b : b + 128] for b in range(0, rows, 128))
            bias_ref[...] = jnp.sum(lanes.T, axis=0, keepdims=True)
            row = lax.broadcasted_iota(jnp.int32, sums_ref.shape, 0)

            def total(keep):
                v = jnp.sum(jnp.where(keep, sums_ref[...], 0.0), axis=0, keepdims=True)
                return jnp.sum(v)

            squares = total(row < 3) / (rows * width)
            active = sparsity_ref[0] * total((row >= 3) & (row < 6)) / (rows * latents * 2 * n)
            loss_ref[0] = squares
            loss_ref[1] = active

        @pl.when(i >= steps)
        def _():
            x = joined(core_ref[0], xa_ref, xb_ref, both_ref)
            enc_ref[...] = lax.dot_general(
                x, g_ref[...], (((1,), (1,)), ((), ())), preferred_element_type=F32
            ).astype(BF)

    first = lambda i: jnp.minimum(i, steps - 1)
    second = lambda i: jnp.maximum(i - steps, 0)
    e_spec = pl.BlockSpec((k, cols + EXTRA, rows), lambda i: (first(i), 0, 0))
    x_spec = pl.BlockSpec((k, cols, rows), lambda i: (second(i), 0, 0))
    tall = pl.BlockSpec((latents, wide), lambda i: (0, first(i)))
    square = whole((latents, rows))
    return pl.pallas_call(
        kernel,
        grid=(2 * steps,),
        in_specs=[SMEM_SPEC, SMEM_SPEC, e_spec, e_spec, x_spec, x_spec, tall, square, square],
        out_specs=[
            tall,
            pl.BlockSpec((wide, latents), lambda i: (second(i), 0)),
            whole((1, latents)),
            SMEM_SPEC,
        ],
        out_shape=[
            jax.ShapeDtypeStruct((latents, width), BF),
            jax.ShapeDtypeStruct((width, latents), BF),
            jax.ShapeDtypeStruct((1, latents), F32),
            jax.ShapeDtypeStruct((2,), F32),
        ],
        scratch_shapes=[
            pltpu.VMEM((latents, rows), F32),
            pltpu.VMEM((latents, rows), BF),
            pltpu.VMEM((k, 2, cols, rows), BF),
            pltpu.VMEM((EXTRA, rows), F32),
        ],
        name="backward",
    )(core, sparsity, e_a, e_b, x_a, x_b, w_dec, feats, slope)


def on_device(inputs, w_enc, b_enc, thresholds, w_dec, b_dec, sparsity):
    n = lax.axis_size("lat_0")
    z = lax.axis_index("lat_0")
    c = lax.axis_index("lat_1")
    core = c.astype(jnp.int32).reshape(1)
    rows, cols = inputs.shape
    latents = w_enc.shape[1]
    x_own = inputs.T

    def half_of(w, k):
        w = w.reshape(n, 2, cols, latents)
        return lax.dynamic_index_in_dim(w, k, 1, False).reshape(n * cols, latents)

    def over_columns(w, a):
        a = a.reshape(n * cols, rows)
        return lax.dot_general(w, a, (((0,), (0,)), ((), ())), preferred_element_type=F32)

    def encoder_halves(token):
        w = after(w_enc, token)
        return half_of(w, c), half_of(w, 1 - c)

    x_a, (w_a, w_b) = gather_chips(x_own, z, n, encoder_halves)
    x_b = swap(x_a)
    pre = over_columns(w_a, x_a) + over_columns(w_b, x_b) + b_enc[:, None]
    gate = jax.nn.sigmoid((pre - thresholds[:, None]) / 0.05)
    feats = (pre * gate).astype(BF)
    count = jnp.sum(gate, axis=0, keepdims=True)

    mine, theirs = decode(core, w_dec, feats, n)
    own, up, down = scatter_sum(mine, swap(theirs), z, n)
    block, grad_b_dec = error_block(own, up, down, x_own, b_dec.astype(F32)[:, None], count)
    e_a, _ = gather_chips(block, z, n)
    slope = gate + pre * gate * (1.0 - gate) / 0.05
    grad_dec, grad_enc, grad_b_enc, loss = backward(
        core, sparsity, e_a, swap(e_a), x_a, x_b, w_dec, feats, slope
    )
    return (grad_enc, grad_b_enc[0], grad_dec, grad_b_dec[:, 0], loss)


def solution(mesh):
    lat = mesh.shape["lat"]
    finer = Mesh(
        mesh.devices.reshape(mesh.shape["groups"], lat // 2, 2), ("groups", "lat_0", "lat_1")
    )
    in_specs = (
        P("groups", LAT),
        P("groups", LAT),
        P(GROUPS_LAT),
        P(GROUPS_LAT),
        P(GROUPS_LAT, None),
        P(GROUPS_LAT),
        P("groups"),
    )
    out_specs = (P("groups", LAT), P(GROUPS_LAT), P(GROUPS_LAT, None), P(GROUPS_LAT), P("groups"))
    return jax.shard_map(
        on_device, mesh=finer, in_specs=in_specs, out_specs=out_specs, check_vma=False
    )
```

```python
import jax
import jax.numpy as jnp
from jax import lax
from jax.experimental import pallas as pl
from jax.experimental.pallas import tpu as pltpu
from jax.sharding import Mesh
from jax.sharding import PartitionSpec as P

LAT = ("lat_0", "lat_1")
GROUPS_LAT = ("groups", "lat_0", "lat_1")
F32 = jnp.float32
BF = jnp.bfloat16


def ring(a, step):
    n = lax.axis_size("lat_0")
    return lax.ppermute(a, "lat_0", [(z, (z + step) % n) for z in range(n)])


def swap(a):
    return lax.ppermute(a, "lat_1", [(0, 1), (1, 0)])


def after(a, b):
    return lax.optimization_barrier((a, b))[0]


def gather_chips(block, z, n, early=None):
    half = n // 2
    full = jnp.zeros((n, *block.shape), block.dtype)

    def store(full, piece, chip):
        return lax.dynamic_update_slice(full, piece[None], (chip % n, 0, 0))

    full = store(full, block, z)
    up = down = last = block
    for k in range(1, half + 1):
        up = after(up, last)
        if early is not None and k == 2:
            up = after(up, early)
        up = ring(up, 1)
        full = store(full, up, z - k)
        last = up
        if k < half:
            down = ring(down, -1)
            full = store(full, down, z + k)
            last = down
    return full


def scatter_sum(mine, theirs, z, n):
    half = n // 2

    def take(chip):
        at = (chip % n, 0, 0)
        size = (1, *mine.shape[1:])
        return (
            lax.dynamic_slice(mine, at, size)[0]
            + lax.dynamic_slice(theirs, at, size)[0].astype(F32)
        )

    up = ring(take(z + half).astype(BF), 1)
    down = ring(take(z - half + 1).astype(BF), -1)
    for j in range(half - 1, 0, -1):
        up, down = lax.optimization_barrier((up, down))
        up = ring((take(z + j) + up.astype(F32)).astype(BF), 1)
        if j > 1:
            down = ring((take(z - j + 1) + down.astype(F32)).astype(BF), -1)
    return take(z), up, down


def joined(c, a_ref, b_ref, both_ref):
    k, _, cols, rows = both_ref.shape
    both_ref[:, pl.ds(c, 1)] = a_ref[:, :cols, :].reshape(k, 1, cols, rows)
    both_ref[:, pl.ds(1 - c, 1)] = b_ref[:, :cols, :].reshape(k, 1, cols, rows)
    return both_ref[...].reshape(2 * k * cols, rows)


def step_chips(n, cols):
    k = 1
    while 2 * k * cols % 128:
        k += 1
    return k


EXTRA = 8
SMEM_SPEC = pl.BlockSpec(memory_space=pltpu.SMEM)


def whole(shape):
    return pl.BlockSpec(shape, lambda i: (0,) * len(shape))


def decode(core, w_dec, feats, n):
    latents, width = w_dec.shape
    rows = feats.shape[1]
    cols = width // (2 * n)
    k = step_chips(n, cols)

    def kernel(core_ref, w_ref, f_ref, mine_ref, theirs_ref, both_ref):
        c = core_ref[0]
        both_ref[...] = lax.dot_general(
            w_ref[...], f_ref[...], (((0,), (0,)), ((), ())), preferred_element_type=F32
        ).reshape(k, 2, cols, rows)
        mine_ref[...] = both_ref[:, pl.ds(c, 1)].reshape(k, cols, rows)
        theirs_ref[...] = both_ref[:, pl.ds(1 - c, 1)].reshape(k, cols, rows).astype(BF)

    block = pl.BlockSpec((k, cols, rows), lambda i: (i, 0, 0))
    return pl.pallas_call(
        kernel,
        grid=(n // k,),
        in_specs=[
            SMEM_SPEC,
            pl.BlockSpec((latents, 2 * k * cols), lambda i: (0, i)),
            whole((latents, rows)),
        ],
        out_specs=[block, block],
        out_shape=[
            jax.ShapeDtypeStruct((n, cols, rows), F32),
            jax.ShapeDtypeStruct((n, cols, rows), BF),
        ],
        scratch_shapes=[pltpu.VMEM((k, 2, cols, rows), F32)],
        name="decode",
    )(core, w_dec, feats)


def error_block(own, up, down, x, bias, count):
    cols, rows = x.shape

    def kernel(own_ref, up_ref, down_ref, x_ref, bias_ref, count_ref, out_ref, grad_ref):
        recon = own_ref[...] + up_ref[...].astype(F32) + down_ref[...].astype(F32)
        err = recon + bias_ref[...] - x_ref[...].astype(F32)
        scaled = 2.0 / rows * err
        out_ref[:cols, :] = scaled.astype(BF)
        grad_ref[...] = jnp.sum(scaled, axis=1, keepdims=True)
        parts = []
        for v in (jnp.sum(err * err, axis=0, keepdims=True), count_ref[...]):
            for _ in range(3):
                part = v.astype(BF)
                parts.append(part.astype(F32))
                v = v - parts[-1]
        row = lax.broadcasted_iota(jnp.int32, (EXTRA, rows), 0)
        extra = jnp.zeros((EXTRA, rows), F32)
        for k, part in enumerate(parts):
            extra = jnp.where(row == k, part, extra)
        out_ref[cols:, :] = extra.astype(BF)

    return pl.pallas_call(
        kernel,
        out_shape=[
            jax.ShapeDtypeStruct((cols + EXTRA, rows), BF),
            jax.ShapeDtypeStruct((cols, 1), F32),
        ],
        compiler_params=pltpu.CompilerParams(vmem_limit_bytes=12 << 20),
        name="error_block",
    )(own, up, down, x, bias, count)


def backward(core, sparsity, e_a, e_b, x_a, x_b, w_dec, feats, slope):
    n, cols, rows = x_a.shape
    latents, width = w_dec.shape
    k = step_chips(n, cols)
    steps = n // k
    wide = 2 * k * cols

    def kernel(
        core_ref, sparsity_ref, ea_ref, eb_ref, xa_ref, xb_ref, w_ref, f_ref, slope_ref,
        dec_ref, enc_ref, bias_ref, loss_ref, acc, g_ref, both_ref, sums_ref,
    ):
        i = pl.program_id(0)

        @pl.when(i == 0)
        def _():
            acc[...] = jnp.zeros_like(acc)
            sums_ref[...] = jnp.zeros_like(sums_ref)

        @pl.when(i < steps)
        def _():
            e = joined(core_ref[0], ea_ref, eb_ref, both_ref)
            dec_ref[...] = lax.dot_general(
                f_ref[...], e, (((1,), (1,)), ((), ())), preferred_element_type=F32
            ).astype(BF)
            acc[...] += jnp.dot(w_ref[...], e, preferred_element_type=F32)
            for q in range(k):
                sums_ref[...] += ea_ref[q, cols:, :].astype(F32) + eb_ref[q, cols:, :].astype(F32)

        @pl.when(i == steps - 1)
        def _():
            g = acc[...] * slope_ref[...]
            g_ref[...] = g.astype(BF)
            lanes = sum(g[:, b : b + 128] for b in range(0, rows, 128))
            bias_ref[...] = jnp.sum(lanes.T, axis=0, keepdims=True)
            row = lax.broadcasted_iota(jnp.int32, sums_ref.shape, 0)

            def total(keep):
                v = jnp.sum(jnp.where(keep, sums_ref[...], 0.0), axis=0, keepdims=True)
                return jnp.sum(v)

            squares = total(row < 3) / (rows * width)
            active = sparsity_ref[0] * total((row >= 3) & (row < 6)) / (rows * latents * 2 * n)
            loss_ref[0] = squares
            loss_ref[1] = active

        @pl.when(i >= steps)
        def _():
            x = joined(core_ref[0], xa_ref, xb_ref, both_ref)
            enc_ref[...] = lax.dot_general(
                x, g_ref[...], (((1,), (1,)), ((), ())), preferred_element_type=F32
            ).astype(BF)

    first = lambda i: jnp.minimum(i, steps - 1)
    second = lambda i: jnp.maximum(i - steps, 0)
    e_spec = pl.BlockSpec((k, cols + EXTRA, rows), lambda i: (first(i), 0, 0))
    x_spec = pl.BlockSpec((k, cols, rows), lambda i: (second(i), 0, 0))
    tall = pl.BlockSpec((latents, wide), lambda i: (0, first(i)))
    square = whole((latents, rows))
    return pl.pallas_call(
        kernel,
        grid=(2 * steps,),
        in_specs=[SMEM_SPEC, SMEM_SPEC, e_spec, e_spec, x_spec, x_spec, tall, square, square],
        out_specs=[
            tall,
            pl.BlockSpec((wide, latents), lambda i: (second(i), 0)),
            whole((1, latents)),
            SMEM_SPEC,
        ],
        out_shape=[
            jax.ShapeDtypeStruct((latents, width), BF),
            jax.ShapeDtypeStruct((width, latents), BF),
            jax.ShapeDtypeStruct((1, latents), F32),
            jax.ShapeDtypeStruct((2,), F32),
        ],
        scratch_shapes=[
            pltpu.VMEM((latents, rows), F32),
            pltpu.VMEM((latents, rows), BF),
            pltpu.VMEM((k, 2, cols, rows), BF),
            pltpu.VMEM((EXTRA, rows), F32),
        ],
        name="backward",
    )(core, sparsity, e_a, e_b, x_a, x_b, w_dec, feats, slope)


def on_device(inputs, w_enc, b_enc, thresholds, w_dec, b_dec, sparsity):
    n = lax.axis_size("lat_0")
    z = lax.axis_index("lat_0")
    c = lax.axis_index("lat_1")
    core = c.astype(jnp.int32).reshape(1)
    rows, cols = inputs.shape
    latents = w_enc.shape[1]
    x_own = inputs.T

    def half_of(w, k):
        w = w.reshape(n, 2, cols, latents)
        return lax.dynamic_index_in_dim(w, k, 1, False).reshape(n * cols, latents)

    def over_columns(w, a):
        a = a.reshape(n * cols, rows)
        return lax.dot_general(w, a, (((0,), (0,)), ((), ())), preferred_element_type=F32)

    w_a, w_b = lax.optimization_barrier((half_of(w_enc, c), half_of(w_enc, 1 - c)))
    x_a = gather_chips(x_own, z, n, (w_a, w_b))
    x_b = swap(x_a)
    pre = lax.optimization_barrier(over_columns(w_a, x_a) + b_enc[:, None])
    pre = pre + over_columns(w_b, x_b)
    gate = jax.nn.sigmoid((pre - thresholds[:, None]) / 0.05)
    feats = (pre * gate).astype(BF)
    count = jnp.sum(gate, axis=0, keepdims=True)

    mine, theirs = decode(core, w_dec, feats, n)
    own, up, down = scatter_sum(mine, swap(theirs), z, n)
    block, grad_b_dec = error_block(own, up, down, x_own, b_dec.astype(F32)[:, None], count)
    e_a = gather_chips(block, z, n)
    slope = gate + pre * gate * (1.0 - gate) / 0.05
    grad_dec, grad_enc, grad_b_enc, loss = backward(
        core, sparsity, e_a, swap(e_a), x_a, x_b, w_dec, feats, slope
    )
    return (grad_enc, grad_b_enc[0], grad_dec, grad_b_dec[:, 0], loss)


def solution(mesh):
    lat = mesh.shape["lat"]
    finer = Mesh(
        mesh.devices.reshape(mesh.shape["groups"], lat // 2, 2), ("groups", "lat_0", "lat_1")
    )
    in_specs = (
        P("groups", LAT),
        P("groups", LAT),
        P(GROUPS_LAT),
        P(GROUPS_LAT),
        P(GROUPS_LAT, None),
        P(GROUPS_LAT),
        P("groups"),
    )
    out_specs = (P("groups", LAT), P(GROUPS_LAT), P(GROUPS_LAT, None), P(GROUPS_LAT), P("groups"))
    return jax.shard_map(
        on_device, mesh=finer, in_specs=in_specs, out_specs=out_specs, check_vma=False
    )
```
